32 devices in a mesh: gx: 2 (over y), gy: 4 (over x, core), gz: 4 (over z).
Axes of the slice: x: 2, y: 2, z: 4, core: 2. Of those that a mesh axis runs over, the one named last changes fastest.
Arguments:
- loads: float32 [16, 4, 16, 1024], P(None, 'gx', 'gy', 'gz'), may hold values from -60 to 60
- moduli: float32 [8], replicated, may hold values from 0.5 to 4
- material: int32 [4, 16, 1024], P('gx', 'gy', 'gz'), may hold values from 0 to 7
Outputs:
- solution: float32 [16, 4, 16, 1024], P(None, 'gx', 'gy', 'gz')
- residual: float32 [16, 4, 16, 1024], P(None, 'gx', 'gy', 'gz')
The draws below stay inside these ranges and needn't reach their ends.
All inputs are finite; a program needn't handle non-finite values.
Results may differ from the reference program's by a relative error of at most 0.005.
The reference program's roundings to bfloat16 on the way (of `kernel`) count: a program that leaves them out, or rounds other values in their place, can miss the bound.
Values may be sent and summed in bfloat16 or wider, within the bound.
A program may use at most 64 MiB of HBM per device.

```python
import math
import jax
import jax.numpy as jnp
import numpy as np
from jax import lax

COLS = 16
MATS = 8
ITERS = 2
NX = 4
NY = 16
NZ = 1024


def draw_loads(key, part):
    key_base = jax.random.fold_in(jax.random.fold_in(key, 11), 0)
    key_scale = jax.random.fold_in(jax.random.fold_in(key, 11), 1)
    key_modes = jax.random.fold_in(jax.random.fold_in(key, 11), 3)
    shape = (COLS, NX, NY, NZ)
    pos_x = jnp.arange(NX, dtype=jnp.float32).reshape(1, NX, 1, 1)
    pos_y = jnp.arange(NY, dtype=jnp.float32).reshape(1, 1, NY, 1)
    pos_z = jnp.arange(NZ, dtype=jnp.float32).reshape(1, 1, 1, NZ)
    depth = pos_z / max(NZ - 1, 1)
    across = pos_x / max(NX - 1, 1)
    upper = (pos_y >= NY // 2).astype(jnp.float32)
    ramp = (1.0 + 2.0 * depth) * 0.5
    roughness = jnp.exp(-math.log(10.0) * (1.2 * upper + 0.4 * across + 0.6 * depth))
    scales = jnp.exp(jax.random.uniform(key_scale, (COLS, 1, 1, 1), jnp.float32, 0.0, math.log(10.0))) / 3.0
    key_my, key_mz, key_coef = jax.random.split(key_modes, 3)
    wave_y = jax.random.randint(key_my, (COLS, 3), 1, 3).astype(jnp.float32)
    wave_z = jax.random.randint(key_mz, (COLS, 3), 1, 5).astype(jnp.float32)
    coefs = jax.random.normal(key_coef, (COLS, 3), jnp.float32)
    shape_x = jnp.sin(math.pi * (pos_x + 1.0) / (NX + 1.0))
    smooth = jnp.zeros(shape, jnp.float32)
    for mode in range(3):
        my = wave_y[:, mode].reshape(COLS, 1, 1, 1)
        mz = wave_z[:, mode].reshape(COLS, 1, 1, 1)
        amp = coefs[:, mode].reshape(COLS, 1, 1, 1)
        term = shape_x * jnp.sin(math.pi * my * (pos_y + 1.0) / (NY + 1.0)) * jnp.sin(math.pi * mz * (pos_z + 1.0) / (NZ + 1.0))
        smooth = smooth + amp * term
    smooth = smooth * math.sqrt(8.0 / 3.0)
    rough = jax.random.normal(key_base, shape, jnp.float32)
    field = roughness * rough + 0.7 * smooth
    return jnp.clip(field * scales * ramp, -60.0, 60.0)


def touch_ends(result, stream_key, least, top_value):
    spot = [jax.random.randint(jax.random.fold_in(stream_key, axis), (), 0, length) for axis, length in enumerate(result.shape)]
    widest = result.shape.index(max(result.shape))
    beside = spot[:widest] + [(spot[widest] + 1) % result.shape[widest]] + spot[widest + 1:]
    return result.at[tuple(spot)].set(least).at[tuple(beside)].set(top_value)


def setup_inputs(seed: int = 0) -> dict:
    arg_keys = jax.random.split(jax.random.key(seed), 4)
    loads = draw_loads(jax.random.fold_in(arg_keys[3], 71), 0)
    moduli = jnp.clip(jnp.exp(jax.random.uniform(arg_keys[1], (MATS,), jnp.float32, math.log(0.5), math.log(4.0))), 0.5, 4.0)
    material = touch_ends(jax.random.randint(arg_keys[2], (NX, NY, NZ), 0, MATS), jax.random.fold_in(arg_keys[2], 1), 0, MATS - 1).astype(jnp.int32)
    return dict(loads=loads, moduli=moduli, material=material)


SIGMA = 0.25

def stiffness_table():
    line_mass = np.array([[1.0 / 3.0, 1.0 / 6.0], [1.0 / 6.0, 1.0 / 3.0]])
    line_stiff = np.array([[1.0, -1.0], [-1.0, 1.0]])
    table = np.zeros((8, 8))
    for target in range(8):
        for source in range(8):
            target_bits = [target >> 2 & 1, target >> 1 & 1, target & 1]
            source_bits = [source >> 2 & 1, source >> 1 & 1, source & 1]
            total = 0.0
            for stiff_dim in range(3):
                factor = 1.0
                for other in range(3):
                    if other == stiff_dim:
                        factor = factor * line_stiff[target_bits[other], source_bits[other]]
                    else:
                        factor = factor * line_mass[target_bits[other], source_bits[other]]
                total = total + factor
            table[target, source] = total
    return table

def corner_bits(corner):
    return (corner >> 2 & 1, corner >> 1 & 1, corner & 1)

def apply_column(column, weights, kernel):
    size_x, size_y, size_z = column.shape
    padded = jnp.pad(column.astype(jnp.bfloat16), 1)
    pieces = []
    for corner in range(8):
        bit_x, bit_y, bit_z = corner_bits(corner)
        pieces.append(padded[bit_x:bit_x + size_x + 1, bit_y:bit_y + size_y + 1, bit_z:bit_z + size_z + 1])
    stacked = jnp.stack(pieces).astype(jnp.float32)
    total = SIGMA * column
    for corner in range(8):
        bit_x, bit_y, bit_z = corner_bits(corner)
        part = jnp.einsum('b,bxyz->xyz', kernel[corner], stacked, precision=lax.Precision.HIGHEST) * weights
        total = total + part[1 - bit_x:1 - bit_x + size_x, 1 - bit_y:1 - bit_y + size_y, 1 - bit_z:1 - bit_z + size_z]
    return total

def gram(left, right):
    return jnp.einsum('cxyz,dxyz->cd', left, right, precision=lax.Precision.HIGHEST)

def combine(block, coeffs):
    return jnp.einsum('cxyz,cd->dxyz', block, coeffs, precision=lax.Precision.HIGHEST)

def solve_small(matrix, rhs_small):
    factor = jnp.linalg.cholesky(matrix)
    return jax.scipy.linalg.cho_solve((factor, True), rhs_small)

def reference(loads, moduli, material):
    kernel = jnp.asarray(stiffness_table(), jnp.float32).astype(jnp.bfloat16).astype(jnp.float32)
    node_modulus = jnp.take(moduli, material, axis=0)
    padded_mod = jnp.pad(node_modulus, 1)
    size_x, size_y, size_z = material.shape
    weights = jnp.zeros((size_x + 1, size_y + 1, size_z + 1), jnp.float32)
    for corner in range(8):
        bit_x, bit_y, bit_z = corner_bits(corner)
        weights = weights + padded_mod[bit_x:bit_x + size_x + 1, bit_y:bit_y + size_y + 1, bit_z:bit_z + size_z + 1]
    weights = weights * 0.125

    def operator(block):
        return lax.map(lambda column: apply_column(column, weights, kernel), block)
    solution = jnp.zeros_like(loads)
    residual = loads
    direction = loads
    current = gram(residual, residual)
    for iteration in range(ITERS):
        image = operator(direction)
        alpha = solve_small(gram(direction, image), current)
        solution = solution + combine(direction, alpha)
        residual = residual - combine(image, alpha)
        if iteration + 1 < ITERS:
            updated = gram(residual, residual)
            beta = solve_small(current, updated)
            direction = residual + combine(direction, beta)
            current = updated
    return (solution, residual)
```

```python
import functools
import itertools

import jax
import jax.numpy as jnp
import numpy as np
from jax import lax
from jax.experimental import pallas as pl
from jax.experimental.pallas import tpu as pltpu
from jax.sharding import PartitionSpec as P

SIGMA = 0.25
AXES = ("gx", "gy", "gz")
HIGH = lax.Precision.HIGHEST
F32 = jnp.float32
BF16 = jnp.bfloat16
LANES = 128
DIRECT_LIMIT = 32


def stiffness_values():
    mass = (1.0 / 3.0, 1.0 / 6.0)
    stiff = (1.0, -1.0)
    values = []
    for differing in range(4):
        bits = [1 if dim < differing else 0 for dim in range(3)]
        total = 0.0
        for dim in range(3):
            factor = 1.0
            for other in range(3):
                factor *= stiff[bits[other]] if other == dim else mass[bits[other]]
            total += factor
        values.append(float(np.asarray(total, np.float32).astype(jnp.bfloat16).astype(np.float32)))
    return values


def dot(left, right, left_dim, right_dim, precision=HIGH):
    return lax.dot_general(
        left, right, (((left_dim,), (right_dim,)), ((), ())), precision=precision, preferred_element_type=F32
    )


def pack(matrix):
    rows = matrix.shape[0]
    wide = jnp.concatenate([matrix, jnp.zeros((rows, LANES - matrix.shape[1]), F32)], axis=1)
    tile = wide[0:8]
    for group in range(1, rows // 8):
        tile = tile + pltpu.roll(wide[8 * group : 8 * group + 8], 32 * group, 1)
    return tile


def unpack(tile):
    pieces = [tile] + [pltpu.roll(tile, LANES - 32 * group, 1) for group in range(1, 4)]
    return jnp.concatenate(pieces, axis=0)[:, 0:32]


def eliminate(matrix, rhs):
    size = matrix.shape[0]
    both = jnp.concatenate([matrix, rhs], axis=1)
    rows = lax.broadcasted_iota(jnp.int32, both.shape, 0)
    for step in range(size):
        pivot_row = both[step : step + 1, :]
        scaled = pivot_row / pivot_row[:, step : step + 1]
        column = both[:, step : step + 1]
        both = jnp.where(rows == step, scaled, both - column * scaled)
    return both[:, size:]


def kernel_body(sizes, phases, stiff, moduli_ref, loads_ref, mat_ref, sol_ref, res_ref,
                stack, padded, sides, padded_im, sides_im, field, wt, wtr, stack2, shares,
                halo_send, halo_recv, sum_send, sum_recv):
    cols = loads_ref.shape[2]
    nx, ny, nz = loads_ref.shape[0], loads_ref.shape[1], loads_ref.shape[3]
    mats = moduli_ref.shape[0]
    me = [lax.axis_index(axis) for axis in AXES]
    k_self, k_edge, k_far = stiff[0], stiff[1], stiff[2]
    assert k_edge == 0.0 and stiff[2] == stiff[3]
    xs, ys = range(nx + 2), range(ny + 2)
    own = list(itertools.product(range(nx), range(ny)))

    directions = [
        d for d in itertools.product((-1, 0, 1), repeat=3)
        if any(d) and all(step == 0 or sizes[i] > 1 for i, step in enumerate(d))
    ]

    def exists(direction):
        good = None
        for i, step in enumerate(direction):
            if step:
                here = (me[i] > 0) if step < 0 else (me[i] < sizes[i] - 1)
                good = here if good is None else jnp.logical_and(good, here)
        return good

    def target(direction):
        return {axis: me[i] + direction[i] for i, axis in enumerate(AXES)}

    def halo_copy(round_, number, core, edge):
        dx, dy, dz = directions[number]
        src_x = {0: pl.ds(1, nx), 1: pl.ds(nx, 1), -1: pl.ds(1, 1)}[dx]
        dst_x = {0: pl.ds(1, nx), 1: pl.ds(0, 1), -1: pl.ds(nx + 1, 1)}[dx]
        src_y = {0: pl.ds(1, ny), 1: pl.ds(ny, 1), -1: pl.ds(1, 1)}[dy]
        dst_y = {0: pl.ds(1, ny), 1: pl.ds(0, 1), -1: pl.ds(ny + 1, 1)}[dy]
        if dz == 0:
            src, dst = core.at[src_x, src_y], core.at[dst_x, dst_y]
        else:
            start = nz - LANES if dz > 0 else 0
            src = core.at[src_x, src_y, :, pl.ds(start, LANES)]
            dst = edge.at[0 if dz > 0 else 1, dst_x, dst_y]
        return pltpu.make_async_remote_copy(
            src_ref=src, dst_ref=dst, send_sem=halo_send.at[round_, number], recv_sem=halo_recv.at[round_, number],
            device_id=target((dx, dy, dz)), device_id_type=pl.DeviceIdType.MESH,
        )

    def halo_start(round_, core, edge):
        for number, direction in enumerate(directions):
            @pl.when(exists(direction))
            def _():
                halo_copy(round_, number, core, edge).start()

    def halo_arrive(round_, core, edge):
        for number, direction in enumerate(directions):
            @pl.when(exists(tuple(-step for step in direction)))
            def _():
                halo_copy(round_, number, core, edge).wait_recv()

    def halo_left(round_, core, edge):
        for number, direction in enumerate(directions):
            @pl.when(exists(direction))
            def _():
                halo_copy(round_, number, core, edge).wait_send()

    def group_of(axes):
        count, index = 1, 0
        for axis in axes:
            i = AXES.index(axis)
            count *= sizes[i]
            index = index * sizes[i] + me[i]
        return count, index

    def peer_id(axes, peer):
        coords = {axis: me[i] for i, axis in enumerate(AXES)}
        for axis in reversed(axes):
            size = sizes[AXES.index(axis)]
            coords[axis] = lax.rem(peer, size)
            peer = lax.div(peer, size)
        return coords

    offsets = []
    total_slots = 0
    for axes in phases:
        offsets.append(total_slots)
        total_slots += group_of(axes)[0]

    for x in xs:
        for y in ys:
            padded[x, y] = jnp.zeros(padded.shape[2:], BF16)
            padded_im[x, y] = jnp.zeros(padded_im.shape[2:], BF16)
            for side in range(2):
                sides[side, x, y] = jnp.zeros(sides.shape[3:], BF16)
                sides_im[side, x, y] = jnp.zeros(sides_im.shape[3:], BF16)

    barrier = pltpu.get_barrier_semaphore()
    expected = 0
    for axes in phases:
        count, index = group_of(axes)

        def greet(k, carry, axes=axes, count=count, index=index):
            pl.semaphore_signal(barrier, inc=1, device_id=peer_id(axes, lax.rem(index + k, count)),
                                device_id_type=pl.DeviceIdType.MESH)
            return carry

        lax.fori_loop(1, count, greet, 0)
        expected = expected + count - 1
    if len(phases) > 1:
        for direction in directions:
            good = exists(direction)

            @pl.when(good)
            def _():
                pl.semaphore_signal(barrier, inc=1, device_id=target(direction),
                                    device_id_type=pl.DeviceIdType.MESH)
            expected = expected + jnp.where(good, 1, 0)

    for x, y in own:
        values = loads_ref[x, y]
        stack[x, y, 0:cols, :] = values
        padded[x + 1, y + 1, 0:cols, :] = values.astype(BF16)
        row = x * ny + y
        ids = (mat_ref[row : row + 1, :] + 1).astype(F32)
        padded[x + 1, y + 1, cols:, :] = jnp.broadcast_to(ids, (cols, nz)).astype(BF16)
    pl.semaphore_wait(barrier, expected)
    halo_start(0, padded, sides)
    halo_arrive(0, padded, sides)

    lane = lax.broadcasted_iota(jnp.int32, (1, LANES), 1)

    def merged(edge, x, y):
        left, right = edge[0, x, y].astype(F32), edge[1, x, y].astype(F32)
        return jnp.where(lane == 0, right, jnp.where(lane == LANES - 1, left, 0.0))

    full = nz + LANES
    moduli = {}
    for x in xs:
        for y in ys:
            tail = merged(sides, x, y)
            everything = jnp.concatenate([padded[x, y].astype(F32), tail], axis=1)
            field[x, y] = everything[0:cols]
            ids = everything[cols : cols + 8]
            modulus = jnp.zeros_like(ids)
            for number in range(mats):
                modulus = modulus + jnp.where(ids == float(number + 1), moduli_ref[number], 0.0)
            moduli[x, y] = modulus
    for x in range(nx + 1):
        for y in range(ny + 1):
            total = (moduli[x, y] + moduli[x, y + 1]) + (moduli[x + 1, y] + moduli[x + 1, y + 1])
            weight = 0.125 * (total + pltpu.roll(total, full - 1, 1))
            wt[x, y] = weight
            wtr[x, y] = pltpu.roll(weight, 1, 1)

    def double(tile):
        return jnp.concatenate([tile, tile], axis=0)

    def operate(direction_of, write):
        for x in range(nx):
            for y in range(ny):
                here = field[x + 1, y + 1]
                ahead = behind = flat = None
                w_ahead = w_behind = None
                for ex in (x, x + 1):
                    for ey in (y, y + 1):
                        corner_sum = (field[ex, ey] + field[ex, ey + 1]) + (field[ex + 1, ey] + field[ex + 1, ey + 1])
                        after, before = wt[ex, ey], wtr[ex, ey]
                        opposite = field[2 * ex - x, 2 * ey - y][:, 0:nz]
                        one = double(before) * corner_sum
                        two = double(after) * corner_sum
                        three = double((before + after)[:, 0:nz]) * opposite
                        ahead = one if ahead is None else ahead + one
                        behind = two if behind is None else behind + two
                        flat = three if flat is None else flat + three
                        w_ahead = before if w_ahead is None else w_ahead + before
                        w_behind = after if w_behind is None else w_behind + after
                ahead = ahead - double(w_ahead) * here
                behind = behind - double(w_behind) * here
                around = pltpu.roll(ahead, full - 1, 1)[:, 0:nz] + pltpu.roll(behind, 1, 1)[:, 0:nz] + flat
                centre = double((w_ahead + w_behind)[:, 0:nz]) * here[:, 0:nz]
                write(x, y, SIGMA * direction_of(x, y) + (k_far * around + k_self * centre))

    def gram(block):
        total = None
        for x, y in own:
            part = dot(block[x, y], block[x, y], 1, 1)
            total = part if total is None else total + part
        return total

    def sum_copy(round_, number, k):
        axes = phases[number]
        count, index = group_of(axes)
        slot = offsets[number] + index
        return pltpu.make_async_remote_copy(
            src_ref=shares.at[round_, slot], dst_ref=shares.at[round_, slot],
            send_sem=sum_send.at[round_, offsets[number] + k], recv_sem=sum_recv.at[round_, offsets[number] + k],
            device_id=peer_id(axes, lax.rem(index + k, count)), device_id_type=pl.DeviceIdType.MESH,
        )

    def sum_arrival(round_, number, k):
        axes = phases[number]
        count, index = group_of(axes)
        source = lax.rem(index + count - k, count)
        slot = offsets[number] + source
        return pltpu.make_async_remote_copy(
            src_ref=shares.at[round_, slot], dst_ref=shares.at[round_, slot],
            send_sem=sum_send.at[round_, offsets[number] + k], recv_sem=sum_recv.at[round_, offsets[number] + k],
            device_id=peer_id(axes, lax.rem(index + k, count)), device_id_type=pl.DeviceIdType.MESH,
        )

    def sum_start(round_, number, tile):
        count, index = group_of(phases[number])
        shares[round_, offsets[number] + index] = tile

        def send(k, carry):
            sum_copy(round_, number, k).start()
            return carry

        lax.fori_loop(1, count, send, 0)

    def sum_finish(round_, number):
        count, _ = group_of(phases[number])

        def receive(k, carry):
            sum_arrival(round_, number, k).wait_recv()
            return carry

        lax.fori_loop(1, count, receive, 0)
        tile = shares[round_, offsets[number]]
        for peer in range(1, count):
            tile = tile + shares[round_, offsets[number] + peer]
        return tile

    def sum_rest(round_):
        tile = sum_finish(round_, 0)
        for number in range(1, len(phases)):
            sum_start(round_, number, tile)
            tile = sum_finish(round_, number)
        return unpack(tile)

    def sum_left(round_):
        for number, axes in enumerate(phases):
            def drain(k, carry, number=number):
                sum_copy(round_, number, k).wait_send()
                return carry

            lax.fori_loop(1, group_of(axes)[0], drain, 0)

    def write_first(x, y, image):
        stack[x, y, cols:, :] = image
        padded_im[x + 1, y + 1] = image.astype(BF16)

    operate(lambda x, y: stack[x, y, 0:cols, :], write_first)
    sum_start(0, 0, pack(gram(stack)))
    halo_start(1, padded_im, sides_im)
    table = sum_rest(0)

    square = table[0:cols, 0:cols]
    curve = 0.5 * (table[0:cols, cols:] + table[cols:, 0:cols])
    row_id = lax.broadcasted_iota(jnp.int32, (cols, cols), 0)
    col_id = lax.broadcasted_iota(jnp.int32, (cols, cols), 1)
    eye = jnp.where(row_id == col_id, 1.0, 0.0)
    alpha = eliminate(curve, square)
    inverse = eliminate(square, eye)
    half = table[:, 0:cols] - dot(table[:, cols:], alpha, 1, 0)
    updated = half[0:cols] - dot(alpha, half[cols:], 0, 0)
    beta = dot(inverse, updated, 1, 0)
    alpha_t = alpha.T
    mix = jnp.concatenate([(eye + beta).T, -alpha_t], axis=1)
    mix_hi = mix.astype(BF16)
    mix_lo = (mix - mix_hi.astype(F32)).astype(BF16)
    mix_both = jnp.concatenate([mix_hi, mix_lo], axis=0)

    halo_arrive(1, padded_im, sides_im)
    for x in xs:
        for y in ys:
            inner = 1 <= x <= nx and 1 <= y <= ny
            tail_l = merged(sides, x, y)[0:cols].astype(BF16)
            tail_i = merged(sides_im, x, y).astype(BF16)
            if inner:
                near = jnp.concatenate([tail_l, tail_i], axis=0)
            else:
                near = jnp.concatenate([
                    jnp.concatenate([padded[x, y, 0:cols, :], tail_l], axis=1),
                    jnp.concatenate([padded_im[x, y], tail_i], axis=1),
                ], axis=0)
            twice = dot(mix_both, near, 1, 0, None)
            mixed = twice[0:cols] + twice[cols:]
            if inner:
                direction = dot(mix, stack[x - 1, y - 1], 1, 0)
                stack2[x - 1, y - 1, 0:cols, :] = direction
                mixed = jnp.concatenate([direction, mixed], axis=1)
            field[x, y] = mixed.astype(BF16).astype(F32)

    def write_second(x, y, image):
        stack2[x, y, cols:, :] = image

    operate(lambda x, y: stack2[x, y, 0:cols, :], write_second)
    sum_start(1, 0, pack(gram(stack2)))
    for x, y in own:
        sol_ref[x, y] = dot(alpha_t, stack[x, y, 0:cols, :], 1, 0)
        res_ref[x, y] = stack[x, y, 0:cols, :] - dot(alpha_t, stack[x, y, cols:, :], 1, 0)
    halo_left(0, padded, sides)
    halo_left(1, padded_im, sides_im)
    sum_left(0)
    table2 = sum_rest(1)
    curve2 = 0.5 * (table2[0:cols, cols:] + table2[cols:, 0:cols])
    alpha2_t = eliminate(curve2, updated).T
    for x, y in own:
        sol_ref[x, y] = sol_ref[x, y] + dot(alpha2_t, stack2[x, y, 0:cols, :], 1, 0)
        res_ref[x, y] = res_ref[x, y] - dot(alpha2_t, stack2[x, y, cols:, :], 1, 0)
    sum_left(1)


def on_device(sizes, loads, moduli, material):
    cols, nx, ny, nz = loads.shape
    count = int(np.prod(sizes))
    phases = (AXES,) if count <= DIRECT_LIMIT else (("gx", "gy"), ("gz",))
    slots = sum(int(np.prod([sizes[AXES.index(a)] for a in axes])) for axes in phases)
    body = functools.partial(kernel_body, sizes, phases, stiffness_values())
    out = jax.ShapeDtypeStruct((nx, ny, cols, nz), F32)
    vmem = pl.BlockSpec(memory_space=pltpu.VMEM)
    full = nz + LANES
    sol, res = pl.pallas_call(
        body,
        out_shape=(out, out),
        in_specs=[pl.BlockSpec(memory_space=pltpu.SMEM), vmem, vmem],
        out_specs=(vmem, vmem),
        scratch_shapes=[
            pltpu.VMEM((nx, ny, 2 * cols, nz), F32),
            pltpu.VMEM((nx + 2, ny + 2, 2 * cols, nz), BF16),
            pltpu.VMEM((2, nx + 2, ny + 2, 2 * cols, LANES), BF16),
            pltpu.VMEM((nx + 2, ny + 2, cols, nz), BF16),
            pltpu.VMEM((2, nx + 2, ny + 2, cols, LANES), BF16),
            pltpu.VMEM((nx + 2, ny + 2, cols, full), F32),
            pltpu.VMEM((nx + 1, ny + 1, 8, full), F32),
            pltpu.VMEM((nx + 1, ny + 1, 8, full), F32),
            pltpu.VMEM((nx, ny, 2 * cols, nz), F32),
            pltpu.VMEM((2, slots, 8, LANES), F32),
            pltpu.SemaphoreType.DMA((2, 26)),
            pltpu.SemaphoreType.DMA((2, 26)),
            pltpu.SemaphoreType.DMA((2, slots)),
            pltpu.SemaphoreType.DMA((2, slots)),
        ],
        compiler_params=pltpu.CompilerParams(collective_id=0, has_side_effects=True),
    )(moduli, loads.transpose(1, 2, 0, 3), material.reshape(nx * ny, nz))
    return sol.transpose(2, 0, 1, 3), res.transpose(2, 0, 1, 3)


def solution(mesh):
    sizes = tuple(mesh.shape[axis] for axis in AXES)
    in_specs = (P(None, "gx", "gy", "gz"), P(), P("gx", "gy", "gz"))
    out_specs = (P(None, "gx", "gy", "gz"), P(None, "gx", "gy", "gz"))
    return jax.shard_map(
        functools.partial(on_device, sizes), mesh=mesh, in_specs=in_specs, out_specs=out_specs, check_vma=False
    )
```

```python
import functools
import itertools

import jax
import jax.numpy as jnp
import numpy as np
from jax import lax
from jax.experimental import pallas as pl
from jax.experimental.pallas import tpu as pltpu
from jax.sharding import PartitionSpec as P

SIGMA = 0.25
AXES = ("gx", "gy", "gz")
HIGH = lax.Precision.HIGHEST
F32 = jnp.float32
BF16 = jnp.bfloat16
LANES = 128
DIRECT_LIMIT = 32


def stiffness_values():
    mass = (1.0 / 3.0, 1.0 / 6.0)
    stiff = (1.0, -1.0)
    values = []
    for differing in range(4):
        bits = [1 if dim < differing else 0 for dim in range(3)]
        total = 0.0
        for dim in range(3):
            factor = 1.0
            for other in range(3):
                factor *= stiff[bits[other]] if other == dim else mass[bits[other]]
            total += factor
        values.append(float(np.asarray(total, np.float32).astype(jnp.bfloat16).astype(np.float32)))
    return values


def dot(left, right, left_dim, right_dim, precision=HIGH):
    return lax.dot_general(
        left, right, (((left_dim,), (right_dim,)), ((), ())), precision=precision, preferred_element_type=F32
    )


def pack(matrix):
    rows = matrix.shape[0]
    wide = jnp.concatenate([matrix, jnp.zeros((rows, LANES - matrix.shape[1]), F32)], axis=1)
    tile = wide[0:8]
    for group in range(1, rows // 8):
        tile = tile + pltpu.roll(wide[8 * group : 8 * group + 8], 32 * group, 1)
    return tile


def unpack(tile):
    pieces = [tile] + [pltpu.roll(tile, LANES - 32 * group, 1) for group in range(1, 4)]
    return jnp.concatenate(pieces, axis=0)[:, 0:32]


def eliminate(matrix, rhs):
    size = matrix.shape[0]
    both = jnp.concatenate([matrix, rhs], axis=1)
    rows = lax.broadcasted_iota(jnp.int32, both.shape, 0)
    for step in range(size):
        pivot_row = both[step : step + 1, :]
        scaled = pivot_row / pivot_row[:, step : step + 1]
        column = both[:, step : step + 1]
        both = jnp.where(rows == step, scaled, both - column * scaled)
    return both[:, size:]


def kernel_body(sizes, phases, stiff, moduli_ref, loads_ref, mat_ref, sol_ref, res_ref,
                stack, padded, sides, padded_im, sides_im, field, wt, wtr, stack2, shares,
                halo_send, halo_recv, sum_send, sum_recv,
                out_stage, local_sems):
    cols, nx, ny, nz = loads_ref.shape
    mats = moduli_ref.shape[0]
    me = [lax.axis_index(axis) for axis in AXES]
    k_self, k_edge, k_far = stiff[0], stiff[1], stiff[2]
    assert k_edge == 0.0 and stiff[2] == stiff[3]
    xs, ys = range(nx + 2), range(ny + 2)
    own = list(itertools.product(range(nx), range(ny)))

    directions = [
        d for d in itertools.product((-1, 0, 1), repeat=3)
        if any(d) and all(step == 0 or sizes[i] > 1 for i, step in enumerate(d))
    ]

    def exists(direction):
        good = None
        for i, step in enumerate(direction):
            if step:
                here = (me[i] > 0) if step < 0 else (me[i] < sizes[i] - 1)
                good = here if good is None else jnp.logical_and(good, here)
        return good

    def target(direction):
        return {axis: me[i] + direction[i] for i, axis in enumerate(AXES)}

    def halo_copy(round_, number, core, edge):
        dx, dy, dz = directions[number]
        src_x = {0: pl.ds(1, nx), 1: pl.ds(nx, 1), -1: pl.ds(1, 1)}[dx]
        dst_x = {0: pl.ds(1, nx), 1: pl.ds(0, 1), -1: pl.ds(nx + 1, 1)}[dx]
        src_y = {0: pl.ds(1, ny), 1: pl.ds(ny, 1), -1: pl.ds(1, 1)}[dy]
        dst_y = {0: pl.ds(1, ny), 1: pl.ds(0, 1), -1: pl.ds(ny + 1, 1)}[dy]
        if dz == 0:
            src, dst = core.at[src_x, src_y], core.at[dst_x, dst_y]
        else:
            start = nz - LANES if dz > 0 else 0
            src = core.at[src_x, src_y, :, pl.ds(start, LANES)]
            dst = edge.at[0 if dz > 0 else 1, dst_x, dst_y]
        return pltpu.make_async_remote_copy(
            src_ref=src, dst_ref=dst, send_sem=halo_send.at[round_, number], recv_sem=halo_recv.at[round_, number],
            device_id=target((dx, dy, dz)), device_id_type=pl.DeviceIdType.MESH,
        )

    def halo_start(round_, core, edge):
        for number, direction in enumerate(directions):
            @pl.when(exists(direction))
            def _():
                halo_copy(round_, number, core, edge).start()

    def halo_arrive(round_, core, edge):
        for number, direction in enumerate(directions):
            @pl.when(exists(tuple(-step for step in direction)))
            def _():
                halo_copy(round_, number, core, edge).wait_recv()

    def halo_left(round_, core, edge):
        for number, direction in enumerate(directions):
            @pl.when(exists(direction))
            def _():
                halo_copy(round_, number, core, edge).wait_send()

    def group_of(axes):
        count, index = 1, 0
        for axis in axes:
            i = AXES.index(axis)
            count *= sizes[i]
            index = index * sizes[i] + me[i]
        return count, index

    def peer_id(axes, peer):
        coords = {axis: me[i] for i, axis in enumerate(AXES)}
        for axis in reversed(axes):
            size = sizes[AXES.index(axis)]
            coords[axis] = lax.rem(peer, size)
            peer = lax.div(peer, size)
        return coords

    offsets = []
    total_slots = 0
    for axes in phases:
        offsets.append(total_slots)
        total_slots += group_of(axes)[0]

    def fetch(x, y):
        return pltpu.make_async_copy(
            loads_ref.at[:, x, y, :], stack.at[x, y, pl.ds(0, cols), :], local_sems.at[0, x * ny + y]
        )

    def put(which, ref, x, y):
        return pltpu.make_async_copy(
            out_stage.at[which, x, y], ref.at[:, x, y, :], local_sems.at[1 + which, x * ny + y]
        )

    for x, y in own:
        fetch(x, y).start()

    for x in xs:
        for y in ys:
            padded[x, y] = jnp.zeros(padded.shape[2:], BF16)
            padded_im[x, y] = jnp.zeros(padded_im.shape[2:], BF16)
            for side in range(2):
                sides[side, x, y] = jnp.zeros(sides.shape[3:], BF16)
                sides_im[side, x, y] = jnp.zeros(sides_im.shape[3:], BF16)

    barrier = pltpu.get_barrier_semaphore()
    expected = 0
    for axes in phases:
        count, index = group_of(axes)

        def greet(k, carry, axes=axes, count=count, index=index):
            pl.semaphore_signal(barrier, inc=1, device_id=peer_id(axes, lax.rem(index + k, count)),
                                device_id_type=pl.DeviceIdType.MESH)
            return carry

        lax.fori_loop(1, count, greet, 0)
        expected = expected + count - 1
    if len(phases) > 1:
        for direction in directions:
            good = exists(direction)

            @pl.when(good)
            def _():
                pl.semaphore_signal(barrier, inc=1, device_id=target(direction),
                                    device_id_type=pl.DeviceIdType.MESH)
            expected = expected + jnp.where(good, 1, 0)

    for x, y in own:
        fetch(x, y).wait()
        values = stack[x, y, 0:cols, :]
        padded[x + 1, y + 1, 0:cols, :] = values.astype(BF16)
        ids = (mat_ref[x, y : y + 1, :] + 1).astype(F32)
        padded[x + 1, y + 1, cols:, :] = jnp.broadcast_to(ids, (cols, nz)).astype(BF16)
    pl.semaphore_wait(barrier, expected)
    halo_start(0, padded, sides)
    halo_arrive(0, padded, sides)

    lane = lax.broadcasted_iota(jnp.int32, (1, LANES), 1)

    def merged(edge, x, y):
        left, right = edge[0, x, y].astype(F32), edge[1, x, y].astype(F32)
        return jnp.where(lane == 0, right, jnp.where(lane == LANES - 1, left, 0.0))

    full = nz + LANES
    moduli = {}
    for x in xs:
        for y in ys:
            tail = merged(sides, x, y)
            everything = jnp.concatenate([padded[x, y].astype(F32), tail], axis=1)
            field[x, y] = everything[0:cols]
            ids = everything[cols : cols + 8]
            modulus = jnp.zeros_like(ids)
            for number in range(mats):
                modulus = modulus + jnp.where(ids == float(number + 1), moduli_ref[number], 0.0)
            moduli[x, y] = modulus
    for x in range(nx + 1):
        for y in range(ny + 1):
            total = (moduli[x, y] + moduli[x, y + 1]) + (moduli[x + 1, y] + moduli[x + 1, y + 1])
            weight = 0.125 * (total + pltpu.roll(total, full - 1, 1))
            wt[x, y] = weight
            wtr[x, y] = pltpu.roll(weight, 1, 1)

    def double(tile):
        return jnp.concatenate([tile, tile], axis=0)

    def operate(direction_of, write):
        for x in range(nx):
            for y in range(ny):
                here = field[x + 1, y + 1]
                ahead = behind = flat = None
                w_ahead = w_behind = None
                for ex in (x, x + 1):
                    for ey in (y, y + 1):
                        corner_sum = (field[ex, ey] + field[ex, ey + 1]) + (field[ex + 1, ey] + field[ex + 1, ey + 1])
                        after, before = wt[ex, ey], wtr[ex, ey]
                        opposite = field[2 * ex - x, 2 * ey - y][:, 0:nz]
                        one = double(before) * corner_sum
                        two = double(after) * corner_sum
                        three = double((before + after)[:, 0:nz]) * opposite
                        ahead = one if ahead is None else ahead + one
                        behind = two if behind is None else behind + two
                        flat = three if flat is None else flat + three
                        w_ahead = before if w_ahead is None else w_ahead + before
                        w_behind = after if w_behind is None else w_behind + after
                ahead = ahead - double(w_ahead) * here
                behind = behind - double(w_behind) * here
                around = pltpu.roll(ahead, full - 1, 1)[:, 0:nz] + pltpu.roll(behind, 1, 1)[:, 0:nz] + flat
                centre = double((w_ahead + w_behind)[:, 0:nz]) * here[:, 0:nz]
                write(x, y, SIGMA * direction_of(x, y) + (k_far * around + k_self * centre))

    def gram(block):
        total = None
        for x, y in own:
            part = dot(block[x, y], block[x, y], 1, 1)
            total = part if total is None else total + part
        return total

    def sum_copy(round_, number, k):
        axes = phases[number]
        count, index = group_of(axes)
        slot = offsets[number] + index
        return pltpu.make_async_remote_copy(
            src_ref=shares.at[round_, slot], dst_ref=shares.at[round_, slot],
            send_sem=sum_send.at[round_, offsets[number] + k], recv_sem=sum_recv.at[round_, offsets[number] + k],
            device_id=peer_id(axes, lax.rem(index + k, count)), device_id_type=pl.DeviceIdType.MESH,
        )

    def sum_arrival(round_, number, k):
        axes = phases[number]
        count, index = group_of(axes)
        source = lax.rem(index + count - k, count)
        slot = offsets[number] + source
        return pltpu.make_async_remote_copy(
            src_ref=shares.at[round_, slot], dst_ref=shares.at[round_, slot],
            send_sem=sum_send.at[round_, offsets[number] + k], recv_sem=sum_recv.at[round_, offsets[number] + k],
            device_id=peer_id(axes, lax.rem(index + k, count)), device_id_type=pl.DeviceIdType.MESH,
        )

    def sum_start(round_, number, tile):
        count, index = group_of(phases[number])
        shares[round_, offsets[number] + index] = tile

        def send(k, carry):
            sum_copy(round_, number, k).start()
            return carry

        lax.fori_loop(1, count, send, 0)

    def sum_finish(round_, number):
        count, _ = group_of(phases[number])

        def receive(k, carry):
            sum_arrival(round_, number, k).wait_recv()
            return carry

        lax.fori_loop(1, count, receive, 0)
        tile = shares[round_, offsets[number]]
        for peer in range(1, count):
            tile = tile + shares[round_, offsets[number] + peer]
        return tile

    def sum_rest(round_):
        tile = sum_finish(round_, 0)
        for number in range(1, len(phases)):
            sum_start(round_, number, tile)
            tile = sum_finish(round_, number)
        return unpack(tile)

    def sum_left(round_):
        for number, axes in enumerate(phases):
            def drain(k, carry, number=number):
                sum_copy(round_, number, k).wait_send()
                return carry

            lax.fori_loop(1, group_of(axes)[0], drain, 0)

    def write_first(x, y, image):
        stack[x, y, cols:, :] = image
        padded_im[x + 1, y + 1] = image.astype(BF16)

    operate(lambda x, y: stack[x, y, 0:cols, :], write_first)
    sum_start(0, 0, pack(gram(stack)))
    halo_start(1, padded_im, sides_im)
    table = sum_rest(0)

    square = table[0:cols, 0:cols]
    curve = 0.5 * (table[0:cols, cols:] + table[cols:, 0:cols])
    row_id = lax.broadcasted_iota(jnp.int32, (cols, cols), 0)
    col_id = lax.broadcasted_iota(jnp.int32, (cols, cols), 1)
    eye = jnp.where(row_id == col_id, 1.0, 0.0)
    alpha = eliminate(curve, square)
    inverse = eliminate(square, eye)
    half = table[:, 0:cols] - dot(table[:, cols:], alpha, 1, 0)
    updated = half[0:cols] - dot(alpha, half[cols:], 0, 0)
    beta = dot(inverse, updated, 1, 0)
    alpha_t = alpha.T
    mix = jnp.concatenate([(eye + beta).T, -alpha_t], axis=1)
    mix_hi = mix.astype(BF16)
    mix_lo = (mix - mix_hi.astype(F32)).astype(BF16)
    mix_both = jnp.concatenate([mix_hi, mix_lo], axis=0)

    halo_arrive(1, padded_im, sides_im)
    for x in xs:
        for y in ys:
            inner = 1 <= x <= nx and 1 <= y <= ny
            tail_l = merged(sides, x, y)[0:cols].astype(BF16)
            tail_i = merged(sides_im, x, y).astype(BF16)
            if inner:
                near = jnp.concatenate([tail_l, tail_i], axis=0)
            else:
                near = jnp.concatenate([
                    jnp.concatenate([padded[x, y, 0:cols, :], tail_l], axis=1),
                    jnp.concatenate([padded_im[x, y], tail_i], axis=1),
                ], axis=0)
            twice = dot(mix_both, near, 1, 0, None)
            mixed = twice[0:cols] + twice[cols:]
            if inner:
                direction = dot(mix, stack[x - 1, y - 1], 1, 0)
                stack2[x - 1, y - 1, 0:cols, :] = direction
                mixed = jnp.concatenate([direction, mixed], axis=1)
            field[x, y] = mixed.astype(BF16).astype(F32)

    def write_second(x, y, image):
        stack2[x, y, cols:, :] = image

    operate(lambda x, y: stack2[x, y, 0:cols, :], write_second)
    sum_start(1, 0, pack(gram(stack2)))
    for x, y in own:
        out_stage[0, x, y] = dot(alpha_t, stack[x, y, 0:cols, :], 1, 0)
        out_stage[1, x, y] = stack[x, y, 0:cols, :] - dot(alpha_t, stack[x, y, cols:, :], 1, 0)
    halo_left(0, padded, sides)
    halo_left(1, padded_im, sides_im)
    sum_left(0)
    table2 = sum_rest(1)
    curve2 = 0.5 * (table2[0:cols, cols:] + table2[cols:, 0:cols])
    alpha2_t = eliminate(curve2, updated).T
    for x, y in own:
        out_stage[0, x, y] = out_stage[0, x, y] + dot(alpha2_t, stack2[x, y, 0:cols, :], 1, 0)
        put(0, sol_ref, x, y).start()
        out_stage[1, x, y] = out_stage[1, x, y] - dot(alpha2_t, stack2[x, y, cols:, :], 1, 0)
        put(1, res_ref, x, y).start()
    sum_left(1)
    for x, y in own:
        put(0, sol_ref, x, y).wait()
        put(1, res_ref, x, y).wait()


def on_device(sizes, loads, moduli, material):
    cols, nx, ny, nz = loads.shape
    count = int(np.prod(sizes))
    phases = (AXES,) if count <= DIRECT_LIMIT else (("gx", "gy"), ("gz",))
    slots = sum(int(np.prod([sizes[AXES.index(a)] for a in axes])) for axes in phases)
    body = functools.partial(kernel_body, sizes, phases, stiffness_values())
    out = jax.ShapeDtypeStruct((cols, nx, ny, nz), F32)
    vmem = pl.BlockSpec(memory_space=pltpu.VMEM)
    anywhere = pl.BlockSpec(memory_space=pl.ANY)
    full = nz + LANES
    return pl.pallas_call(
        body,
        out_shape=(out, out),
        in_specs=[pl.BlockSpec(memory_space=pltpu.SMEM), anywhere, vmem],
        out_specs=(anywhere, anywhere),
        scratch_shapes=[
            pltpu.VMEM((nx, ny, 2 * cols, nz), F32),
            pltpu.VMEM((nx + 2, ny + 2, 2 * cols, nz), BF16),
            pltpu.VMEM((2, nx + 2, ny + 2, 2 * cols, LANES), BF16),
            pltpu.VMEM((nx + 2, ny + 2, cols, nz), BF16),
            pltpu.VMEM((2, nx + 2, ny + 2, cols, LANES), BF16),
            pltpu.VMEM((nx + 2, ny + 2, cols, full), F32),
            pltpu.VMEM((nx + 1, ny + 1, 8, full), F32),
            pltpu.VMEM((nx + 1, ny + 1, 8, full), F32),
            pltpu.VMEM((nx, ny, 2 * cols, nz), F32),
            pltpu.VMEM((2, slots, 8, LANES), F32),
            pltpu.SemaphoreType.DMA((2, 26)),
            pltpu.SemaphoreType.DMA((2, 26)),
            pltpu.SemaphoreType.DMA((2, slots)),
            pltpu.SemaphoreType.DMA((2, slots)),
            pltpu.VMEM((2, nx, ny, cols, nz), F32),
            pltpu.SemaphoreType.DMA((3, nx * ny)),
        ],
        compiler_params=pltpu.CompilerParams(collective_id=0, has_side_effects=True),
    )(moduli, loads, material)


def solution(mesh):
    sizes = tuple(mesh.shape[axis] for axis in AXES)
    in_specs = (P(None, "gx", "gy", "gz"), P(), P("gx", "gy", "gz"))
    out_specs = (P(None, "gx", "gy", "gz"), P(None, "gx", "gy", "gz"))
    return jax.shard_map(
        functools.partial(on_device, sizes), mesh=mesh, in_specs=in_specs, out_specs=out_specs, check_vma=False
    )
```

```python
import functools
import itertools

import jax
import jax.numpy as jnp
import numpy as np
from jax import lax
from jax.experimental import pallas as pl
from jax.experimental.pallas import tpu as pltpu
from jax.sharding import PartitionSpec as P

SIGMA = 0.25
AXES = ("gx", "gy", "gz")
HIGH = lax.Precision.HIGHEST
F32 = jnp.float32
BF16 = jnp.bfloat16
LANES = 128
DIRECT_LIMIT = 32


def stiffness_values():
    mass = (1.0 / 3.0, 1.0 / 6.0)
    stiff = (1.0, -1.0)
    values = []
    for differing in range(4):
        bits = [1 if dim < differing else 0 for dim in range(3)]
        total = 0.0
        for dim in range(3):
            factor = 1.0
            for other in range(3):
                factor *= stiff[bits[other]] if other == dim else mass[bits[other]]
            total += factor
        values.append(float(np.asarray(total, np.float32).astype(jnp.bfloat16).astype(np.float32)))
    return values


def dot(left, right, left_dim, right_dim, precision=HIGH):
    return lax.dot_general(
        left, right, (((left_dim,), (right_dim,)), ((), ())), precision=precision, preferred_element_type=F32
    )


def pack(matrix):
    rows, cols = matrix.shape
    wide = jnp.concatenate([matrix, jnp.zeros((rows, LANES - cols), F32)], axis=1)
    pieces = [
        jnp.sum(pltpu.roll(wide[start : start + 8], 0, 1, stride=cols, stride_axis=0), axis=0, keepdims=True)
        for start in range(0, rows, 8)
    ]
    return jnp.concatenate(pieces, axis=0)


def unpack(tile, cols):
    rows = tile.shape[0]
    tall = jnp.concatenate([tile, jnp.zeros((8 - rows, LANES), F32)], axis=0)
    turned = [tall] + [pltpu.roll(tall, LANES - cols * group, 1) for group in range(1, 8)]
    return jnp.concatenate(
        [turned[group][row : row + 1] for row in range(rows) for group in range(8)], axis=0
    )[:, 0:cols]


def eliminate(matrix, rhs):
    size = matrix.shape[0]
    both = jnp.concatenate([matrix, rhs], axis=1)
    rows = lax.broadcasted_iota(jnp.int32, both.shape, 0)
    for step in range(0, size, 2):
        top, low = both[step : step + 1, :], both[step + 1 : step + 2, :]
        left, right = both[:, step : step + 1], both[:, step + 1 : step + 2]
        first, mixed, second = top[:, step : step + 1], top[:, step + 1 : step + 2], low[:, step + 1 : step + 2]
        ratio = mixed / first
        low_new = (low - ratio * top) / (second - ratio * mixed)
        top_new = top / first - ratio * low_new
        rest = both - left * top_new - right * low_new
        both = jnp.where(rows == step, top_new, jnp.where(rows == step + 1, low_new, rest))
    return both[:, size:]


def kernel_body(sizes, phases, stiff, moduli_ref, loads_ref, mat_ref, sol_ref, res_ref,
                stack, padded, padded_im, mats_rx, ends, ends_rx, ends_im, ends_im_rx, field, wt, wtr, stack2,
                shares_rr, shares_im, shares_last, halo_send, halo_recv, sum_send, sum_recv,
                out_stage, local_sems):
    cols, nx, ny, nz = loads_ref.shape
    mats = moduli_ref.shape[0]
    me = [lax.axis_index(axis) for axis in AXES]
    k_self, k_edge, k_far = stiff[0], stiff[1], stiff[2]
    assert k_edge == 0.0 and stiff[2] == stiff[3]
    xs, ys = range(nx + 2), range(ny + 2)
    shares_of = (shares_rr, shares_im, shares_last)
    own = list(itertools.product(range(nx), range(ny)))

    directions = [
        d for d in itertools.product((-1, 0, 1), repeat=3)
        if any(d) and all(step == 0 or sizes[i] > 1 for i, step in enumerate(d))
    ]

    def exists(direction):
        good = None
        for i, step in enumerate(direction):
            if step:
                here = (me[i] > 0) if step < 0 else (me[i] < sizes[i] - 1)
                good = here if good is None else jnp.logical_and(good, here)
        return good

    def target(direction):
        return {axis: me[i] + direction[i] for i, axis in enumerate(AXES)}

    def place(direction):
        return 1 - direction[0], 1 - direction[1]

    def halo_copies(round_, number):
        direction = dx, dy, dz = directions[number]
        core, source, edge = ((padded, ends, ends_rx), (padded_im, ends_im, ends_im_rx))[round_]
        pairs = []
        if dz == 0:
            src_x = {0: pl.ds(1, nx), 1: pl.ds(nx, 1), -1: pl.ds(1, 1)}[dx]
            dst_x = {0: pl.ds(1, nx), 1: pl.ds(0, 1), -1: pl.ds(nx + 1, 1)}[dx]
            src_y = {0: pl.ds(1, ny), 1: pl.ds(ny, 1), -1: pl.ds(1, 1)}[dy]
            dst_y = {0: pl.ds(1, ny), 1: pl.ds(0, 1), -1: pl.ds(ny + 1, 1)}[dy]
            pairs.append((core.at[src_x, src_y], core.at[dst_x, dst_y]))
            if round_ == 0:
                pairs.append((mats_rx.at[1, 1], mats_rx.at[place(direction)]))
        else:
            pairs.append((source.at[1 if dz > 0 else 0], edge.at[(*place(direction), 0 if dz > 0 else 1)]))
        return [
            pltpu.make_async_remote_copy(
                src_ref=src, dst_ref=dst, send_sem=halo_send.at[round_ + 2 * i, number],
                recv_sem=halo_recv.at[round_ + 2 * i, number],
                device_id=target(direction), device_id_type=pl.DeviceIdType.MESH,
            )
            for i, (src, dst) in enumerate(pairs)
        ]

    def halo_each(round_, act, incoming=False):
        for number, direction in enumerate(directions):
            @pl.when(exists(tuple(-step for step in direction) if incoming else direction))
            def _():
                for copy in halo_copies(round_, number):
                    act(copy)

    def halo_start(round_):
        halo_each(round_, lambda copy: copy.start())

    def halo_arrive(round_):
        halo_each(round_, lambda copy: copy.wait_recv(), True)

    def halo_left(round_):
        halo_each(round_, lambda copy: copy.wait_send())

    def each(count, body):
        if count <= 8:
            for k in range(1, count):
                body(k, 0)
        else:
            lax.fori_loop(1, count, body, 0)

    def group_of(axes):
        count, index = 1, 0
        for axis in axes:
            i = AXES.index(axis)
            count *= sizes[i]
            index = index * sizes[i] + me[i]
        return count, index

    def peer_id(axes, peer):
        coords = {axis: me[i] for i, axis in enumerate(AXES)}
        for axis in reversed(axes):
            size = sizes[AXES.index(axis)]
            coords[axis] = lax.rem(peer, size)
            peer = lax.div(peer, size)
        return coords

    offsets = []
    total_slots = 0
    for axes in phases:
        offsets.append(total_slots)
        total_slots += group_of(axes)[0]

    def fetch(x, y):
        return pltpu.make_async_copy(
            loads_ref.at[:, x, y, :], stack.at[x, y, pl.ds(0, cols), :], local_sems.at[0, x * ny + y]
        )

    def put(which, ref, x, y):
        return pltpu.make_async_copy(
            out_stage.at[which, x, y], ref.at[:, x, y, :], local_sems.at[1 + which, x * ny + y]
        )

    for x, y in own:
        fetch(x, y).start()

    for x in xs:
        for y in ys:
            if not (1 <= x <= nx and 1 <= y <= ny):
                padded[x, y] = jnp.zeros(padded.shape[2:], BF16)
                padded_im[x, y] = jnp.zeros(padded_im.shape[2:], BF16)
    for bx, by in itertools.product(range(3), repeat=2):
        mats_rx[bx, by] = jnp.zeros(mats_rx.shape[2:], F32)
        for side in range(2):
            ends_rx[bx, by, side] = jnp.zeros(ends_rx.shape[3:], BF16)
            ends_im_rx[bx, by, side] = jnp.zeros(ends_im_rx.shape[3:], BF16)

    barrier = pltpu.get_barrier_semaphore()
    expected = 0
    for axes in phases:
        count, index = group_of(axes)

        def greet(k, carry, axes=axes, count=count, index=index):
            pl.semaphore_signal(barrier, inc=1, device_id=peer_id(axes, lax.rem(index + k, count)),
                                device_id_type=pl.DeviceIdType.MESH)
            return carry

        each(count, greet)
        expected = expected + count - 1
    if len(phases) > 1:
        for direction in directions:
            good = exists(direction)

            @pl.when(good)
            def _():
                pl.semaphore_signal(barrier, inc=1, device_id=target(direction),
                                    device_id_type=pl.DeviceIdType.MESH)
            expected = expected + jnp.where(good, 1, 0)

    lane = lax.broadcasted_iota(jnp.int32, (1, LANES), 1)
    firsts = lasts = jnp.zeros((2 * cols, LANES), F32)
    for x in range(nx):
        mats_rx[1, 1, x * ny : (x + 1) * ny, :] = (mat_ref[x] + 1).astype(F32)
    for x, y in own:
        fetch(x, y).wait()
        values = stack[x, y, 0:cols, :]
        padded[x + 1, y + 1] = values.astype(BF16)
        row = x * ny + y
        ids = jnp.broadcast_to(mats_rx[1, 1, row : row + 1, :], (cols, nz))
        column = jnp.concatenate([values, ids], axis=0)
        firsts = jnp.where(lane == row, column[:, 0:1], firsts)
        lasts = jnp.where(lane == row, column[:, nz - 1 : nz], lasts)
    ends[0] = firsts.astype(BF16)
    ends[1] = lasts.astype(BF16)
    pl.semaphore_wait(barrier, expected)
    halo_start(0)

    def block_of(x, y):
        bx, lx = (0, nx - 1) if x == 0 else (2, 0) if x == nx + 1 else (1, x - 1)
        by, ly = (0, ny - 1) if y == 0 else (2, 0) if y == ny + 1 else (1, y - 1)
        return bx, by, lx * ny + ly

    def merged(edge, x, y):
        bx, by, row = block_of(x, y)
        left, right = edge[bx, by, 0].astype(F32), edge[bx, by, 1].astype(F32)
        return jnp.where(lane == 0, right[:, row : row + 1],
                         jnp.where(lane == LANES - 1, left[:, row : row + 1], 0.0))

    def gram(left, right):
        total = None
        for x, y in own:
            part = dot(left(x, y), right(x, y), 1, 1)
            total = part if total is None else total + part
        return total

    def sum_copy(round_, number, k):
        axes = phases[number]
        count, index = group_of(axes)
        slot = offsets[number] + index
        return pltpu.make_async_remote_copy(
            src_ref=shares_of[round_].at[slot], dst_ref=shares_of[round_].at[slot],
            send_sem=sum_send.at[round_, offsets[number] + k], recv_sem=sum_recv.at[round_, offsets[number] + k],
            device_id=peer_id(axes, lax.rem(index + k, count)), device_id_type=pl.DeviceIdType.MESH,
        )

    def sum_arrival(round_, number, k):
        axes = phases[number]
        count, index = group_of(axes)
        source = lax.rem(index + count - k, count)
        slot = offsets[number] + source
        return pltpu.make_async_remote_copy(
            src_ref=shares_of[round_].at[slot], dst_ref=shares_of[round_].at[slot],
            send_sem=sum_send.at[round_, offsets[number] + k], recv_sem=sum_recv.at[round_, offsets[number] + k],
            device_id=peer_id(axes, lax.rem(index + k, count)), device_id_type=pl.DeviceIdType.MESH,
        )

    def sum_start(round_, number, tile):
        count, index = group_of(phases[number])
        shares_of[round_][offsets[number] + index] = tile

        def send(k, carry):
            sum_copy(round_, number, k).start()
            return carry

        each(count, send)

    def sum_finish(round_, number):
        count, _ = group_of(phases[number])

        def receive(k, carry):
            sum_arrival(round_, number, k).wait_recv()
            return carry

        each(count, receive)
        tile = shares_of[round_][offsets[number]]
        for peer in range(1, count):
            tile = tile + shares_of[round_][offsets[number] + peer]
        return tile

    def sum_turn(round_):
        for number in range(1, len(phases)):
            sum_start(round_, number, sum_finish(round_, number - 1))

    def sum_rest(round_):
        return unpack(sum_finish(round_, len(phases) - 1), cols)

    def sum_left(round_):
        for number, axes in enumerate(phases):
            def drain(k, carry, number=number):
                sum_copy(round_, number, k).wait_send()
                return carry

            each(group_of(axes)[0], drain)

    def loads_at(x, y):
        return stack[x, y, 0:cols, :]

    def image_at(x, y):
        return stack[x, y, cols:, :]

    def loads_at2(x, y):
        return stack2[x, y, 0:cols, :]

    def image_at2(x, y):
        return stack2[x, y, cols:, :]

    sum_start(0, 0, pack(gram(loads_at, loads_at)))
    halo_arrive(0)
    sum_turn(0)
    full = nz + LANES
    moduli = {}
    for x in xs:
        for y in ys:
            tail = merged(ends_rx, x, y)
            field[x, y] = jnp.concatenate([padded[x, y].astype(F32), tail[0:cols]], axis=1)
            bx, by, row = block_of(x, y)
            ids = jnp.concatenate([
                jnp.broadcast_to(mats_rx[bx, by, row : row + 1, :], (8, nz)), tail[cols : cols + 8]
            ], axis=1)
            modulus = jnp.zeros_like(ids)
            for number in range(mats):
                modulus = modulus + jnp.where(ids == float(number + 1), moduli_ref[number], 0.0)
            moduli[x, y] = modulus
    for x in range(nx + 1):
        for y in range(ny + 1):
            total = (moduli[x, y] + moduli[x, y + 1]) + (moduli[x + 1, y] + moduli[x + 1, y + 1])
            weight = 0.125 * (total + pltpu.roll(total, full - 1, 1))
            wt[x, y] = weight
            wtr[x, y] = pltpu.roll(weight, 1, 1)

    def double(tile):
        return jnp.concatenate([tile, tile], axis=0)

    def operate(direction_of, write):
        for x in range(nx):
            for y in range(ny):
                here = field[x + 1, y + 1]
                ahead = behind = flat = None
                w_ahead = w_behind = None
                for ex in (x, x + 1):
                    for ey in (y, y + 1):
                        corner_sum = (field[ex, ey] + field[ex, ey + 1]) + (field[ex + 1, ey] + field[ex + 1, ey + 1])
                        after, before = wt[ex, ey], wtr[ex, ey]
                        opposite = field[2 * ex - x, 2 * ey - y][:, 0:nz]
                        one = double(before) * corner_sum
                        two = double(after) * corner_sum
                        three = double((before + after)[:, 0:nz]) * opposite
                        ahead = one if ahead is None else ahead + one
                        behind = two if behind is None else behind + two
                        flat = three if flat is None else flat + three
                        w_ahead = before if w_ahead is None else w_ahead + before
                        w_behind = after if w_behind is None else w_behind + after
                ahead = ahead - double(w_ahead) * here
                behind = behind - double(w_behind) * here
                around = pltpu.roll(ahead, full - 1, 1)[:, 0:nz] + pltpu.roll(behind, 1, 1)[:, 0:nz] + flat
                centre = double((w_ahead + w_behind)[:, 0:nz]) * here[:, 0:nz]
                write(x, y, SIGMA * direction_of(x, y) + (k_far * around + k_self * centre))

    image_firsts = jnp.zeros((cols, LANES), F32)
    image_ends = [image_firsts, image_firsts]

    def write_first(x, y, image):
        stack[x, y, cols:, :] = image
        padded_im[x + 1, y + 1] = image.astype(BF16)
        row = x * ny + y
        image_ends[0] = jnp.where(lane == row, image[:, 0:1], image_ends[0])
        image_ends[1] = jnp.where(lane == row, image[:, nz - 1 : nz], image_ends[1])

    operate(loads_at, write_first)
    ends_im[0] = image_ends[0].astype(BF16)
    ends_im[1] = image_ends[1].astype(BF16)
    cross_part = gram(image_at, lambda x, y: stack[x, y])
    sum_start(1, 0, jnp.concatenate([pack(cross_part[:, 0:cols]), pack(cross_part[:, cols:])], axis=0))
    halo_start(1)
    square = sum_rest(0)
    sum_turn(1)
    row_id = lax.broadcasted_iota(jnp.int32, (cols, cols), 0)
    col_id = lax.broadcasted_iota(jnp.int32, (cols, cols), 1)
    eye = jnp.where(row_id == col_id, 1.0, 0.0)
    inverse = eliminate(square, eye)
    table = sum_rest(1)

    cross, quad = table[0:cols], table[cols:]
    alpha = eliminate(0.5 * (cross + cross.T), square)
    updated = square + dot(alpha, dot(quad, alpha, 1, 0) - cross, 0, 0) - dot(cross, alpha, 0, 0)
    beta = dot(inverse, updated, 1, 0)
    alpha_t = alpha.T
    mix = jnp.concatenate([(eye + beta).T, -alpha_t], axis=1)
    mix_hi = mix.astype(BF16)
    mix_lo = (mix - mix_hi.astype(F32)).astype(BF16)
    mix_both = jnp.concatenate([mix_hi, mix_lo], axis=0)

    halo_arrive(1)
    for x in xs:
        for y in ys:
            inner = 1 <= x <= nx and 1 <= y <= ny
            tail_l = merged(ends_rx, x, y)[0:cols].astype(BF16)
            tail_i = merged(ends_im_rx, x, y).astype(BF16)
            if inner:
                near = jnp.concatenate([tail_l, tail_i], axis=0)
            else:
                near = jnp.concatenate([
                    jnp.concatenate([padded[x, y], tail_l], axis=1),
                    jnp.concatenate([padded_im[x, y], tail_i], axis=1),
                ], axis=0)
            twice = dot(mix_both, near, 1, 0, None)
            mixed = twice[0:cols] + twice[cols:]
            if inner:
                direction = dot(mix, stack[x - 1, y - 1], 1, 0)
                stack2[x - 1, y - 1, 0:cols, :] = direction
                mixed = jnp.concatenate([direction, mixed], axis=1)
            field[x, y] = mixed.astype(BF16).astype(F32)

    def write_second(x, y, image):
        stack2[x, y, cols:, :] = image

    operate(loads_at2, write_second)
    sum_start(2, 0, pack(gram(image_at2, loads_at2)))
    for x, y in own:
        out_stage[0, x, y] = dot(alpha_t, stack[x, y, 0:cols, :], 1, 0)
        out_stage[1, x, y] = stack[x, y, 0:cols, :] - dot(alpha_t, stack[x, y, cols:, :], 1, 0)
    halo_left(0)
    halo_left(1)
    sum_left(0)
    sum_left(1)
    sum_turn(2)
    cross2 = sum_rest(2)
    alpha2_t = eliminate(0.5 * (cross2 + cross2.T), updated).T
    for x, y in own:
        out_stage[0, x, y] = out_stage[0, x, y] + dot(alpha2_t, stack2[x, y, 0:cols, :], 1, 0)
        put(0, sol_ref, x, y).start()
        out_stage[1, x, y] = out_stage[1, x, y] - dot(alpha2_t, stack2[x, y, cols:, :], 1, 0)
        put(1, res_ref, x, y).start()
    sum_left(2)
    for x, y in own:
        put(0, sol_ref, x, y).wait()
        put(1, res_ref, x, y).wait()


def on_device(sizes, loads, moduli, material):
    cols, nx, ny, nz = loads.shape
    count = int(np.prod(sizes))
    phases = (AXES,) if count <= DIRECT_LIMIT else (("gx", "gy"), ("gz",))
    slots = sum(int(np.prod([sizes[AXES.index(a)] for a in axes])) for axes in phases)
    body = functools.partial(kernel_body, sizes, phases, stiffness_values())
    out = jax.ShapeDtypeStruct((cols, nx, ny, nz), F32)
    vmem = pl.BlockSpec(memory_space=pltpu.VMEM)
    anywhere = pl.BlockSpec(memory_space=pl.ANY)
    full = nz + LANES
    return pl.pallas_call(
        body,
        out_shape=(out, out),
        in_specs=[pl.BlockSpec(memory_space=pltpu.SMEM), anywhere, vmem],
        out_specs=(anywhere, anywhere),
        scratch_shapes=[
            pltpu.VMEM((nx, ny, 2 * cols, nz), F32),
            pltpu.VMEM((nx + 2, ny + 2, cols, nz), BF16),
            pltpu.VMEM((nx + 2, ny + 2, cols, nz), BF16),
            pltpu.VMEM((3, 3, nx * ny, nz), F32),
            pltpu.VMEM((2, 2 * cols, LANES), BF16),
            pltpu.VMEM((3, 3, 2, 2 * cols, LANES), BF16),
            pltpu.VMEM((2, cols, LANES), BF16),
            pltpu.VMEM((3, 3, 2, cols, LANES), BF16),
            pltpu.VMEM((nx + 2, ny + 2, cols, full), F32),
            pltpu.VMEM((nx + 1, ny + 1, 8, full), F32),
            pltpu.VMEM((nx + 1, ny + 1, 8, full), F32),
            pltpu.VMEM((nx, ny, 2 * cols, nz), F32),
            pltpu.VMEM((slots, cols * cols // LANES, LANES), F32),
            pltpu.VMEM((slots, 2 * cols * cols // LANES, LANES), F32),
            pltpu.VMEM((slots, cols * cols // LANES, LANES), F32),
            pltpu.SemaphoreType.DMA((3, 26)),
            pltpu.SemaphoreType.DMA((3, 26)),
            pltpu.SemaphoreType.DMA((3, slots)),
            pltpu.SemaphoreType.DMA((3, slots)),
            pltpu.VMEM((2, nx, ny, cols, nz), F32),
            pltpu.SemaphoreType.DMA((3, nx * ny)),
        ],
        compiler_params=pltpu.CompilerParams(collective_id=0, has_side_effects=True),
    )(moduli, loads, material)


def solution(mesh):
    sizes = tuple(mesh.shape[axis] for axis in AXES)
    in_specs = (P(None, "gx", "gy", "gz"), P(), P("gx", "gy", "gz"))
    out_specs = (P(None, "gx", "gy", "gz"), P(None, "gx", "gy", "gz"))
    return jax.shard_map(
        functools.partial(on_device, sizes), mesh=mesh, in_specs=in_specs, out_specs=out_specs, check_vma=False
    )
```

```python
import functools
import itertools

import jax
import jax.numpy as jnp
import numpy as np
from jax import lax
from jax.experimental import pallas as pl
from jax.experimental.pallas import tpu as pltpu
from jax.sharding import PartitionSpec as P

SIGMA = 0.25
AXES = ("gx", "gy", "gz")
HIGH = lax.Precision.HIGHEST
F32 = jnp.float32
BF16 = jnp.bfloat16
LANES = 128
DIRECT_LIMIT = 32


def stiffness_values():
    mass = (1.0 / 3.0, 1.0 / 6.0)
    stiff = (1.0, -1.0)
    values = []
    for differing in range(4):
        bits = [1 if dim < differing else 0 for dim in range(3)]
        total = 0.0
        for dim in range(3):
            factor = 1.0
            for other in range(3):
                factor *= stiff[bits[other]] if other == dim else mass[bits[other]]
            total += factor
        values.append(float(np.asarray(total, np.float32).astype(jnp.bfloat16).astype(np.float32)))
    return values


def dot(left, right, left_dim, right_dim, precision=HIGH):
    return lax.dot_general(
        left, right, (((left_dim,), (right_dim,)), ((), ())), precision=precision, preferred_element_type=F32
    )


def pack(matrix):
    rows, cols = matrix.shape
    wide = jnp.concatenate([matrix, jnp.zeros((rows, LANES - cols), F32)], axis=1)
    pieces = [
        jnp.sum(pltpu.roll(wide[start : start + 8], 0, 1, stride=cols, stride_axis=0), axis=0, keepdims=True)
        for start in range(0, rows, 8)
    ]
    return jnp.concatenate(pieces, axis=0)


def unpack(tile, cols):
    rows = tile.shape[0]
    tall = jnp.concatenate([tile, jnp.zeros((8 - rows, LANES), F32)], axis=0)
    turned = [tall] + [pltpu.roll(tall, LANES - cols * group, 1) for group in range(1, 8)]
    return jnp.concatenate(
        [turned[group][row : row + 1] for row in range(rows) for group in range(8)], axis=0
    )[:, 0:cols]


def eliminate(matrix, rhs):
    size = matrix.shape[0]
    both = jnp.concatenate([matrix, rhs], axis=1)
    rows = lax.broadcasted_iota(jnp.int32, both.shape, 0)
    for step in range(0, size, 2):
        top, low = both[step : step + 1, :], both[step + 1 : step + 2, :]
        left, right = both[:, step : step + 1], both[:, step + 1 : step + 2]
        first, mixed, second = top[:, step : step + 1], top[:, step + 1 : step + 2], low[:, step + 1 : step + 2]
        ratio = mixed / first
        low_new = (low - ratio * top) / (second - ratio * mixed)
        top_new = top / first - ratio * low_new
        rest = both - left * top_new - right * low_new
        both = jnp.where(rows == step, top_new, jnp.where(rows == step + 1, low_new, rest))
    return both[:, size:]


def kernel_body(sizes, phases, stiff, moduli_ref, loads_ref, mat_ref, sol_ref, res_ref,
                stack, padded, padded_im, mats_rx, ends, ends_rx, ends_im, ends_im_rx, field, wt, wtr, stack2,
                shares_rr, shares_im, shares_last, halo_send, halo_recv, sum_send, sum_recv,
                out_stage, local_sems, vouch_sem):
    cols, nx, ny, nz = loads_ref.shape
    mats = moduli_ref.shape[0]
    me = [lax.axis_index(axis) for axis in AXES]
    k_self, k_edge, k_far = stiff[0], stiff[1], stiff[2]
    assert k_edge == 0.0 and stiff[2] == stiff[3]
    xs, ys = range(nx + 2), range(ny + 2)
    shares_of = (shares_rr, shares_im, shares_last)
    own = list(itertools.product(range(nx), range(ny)))

    directions = [
        d for d in itertools.product((-1, 0, 1), repeat=3)
        if any(d) and all(step == 0 or sizes[i] > 1 for i, step in enumerate(d))
    ]

    def exists(direction):
        good = None
        for i, step in enumerate(direction):
            if step:
                here = (me[i] > 0) if step < 0 else (me[i] < sizes[i] - 1)
                good = here if good is None else jnp.logical_and(good, here)
        return good

    def target(direction):
        return {axis: me[i] + direction[i] for i, axis in enumerate(AXES)}

    def place(direction):
        return 1 - direction[0], 1 - direction[1]

    def halo_copies(round_, number):
        direction = dx, dy, dz = directions[number]
        core, source, edge = ((padded, ends, ends_rx), (padded_im, ends_im, ends_im_rx))[round_]
        pairs = []
        if dz == 0:
            src_x = {0: pl.ds(1, nx), 1: pl.ds(nx, 1), -1: pl.ds(1, 1)}[dx]
            dst_x = {0: pl.ds(1, nx), 1: pl.ds(0, 1), -1: pl.ds(nx + 1, 1)}[dx]
            src_y = {0: pl.ds(1, ny), 1: pl.ds(ny, 1), -1: pl.ds(1, 1)}[dy]
            dst_y = {0: pl.ds(1, ny), 1: pl.ds(0, 1), -1: pl.ds(ny + 1, 1)}[dy]
            pairs.append((core.at[src_x, src_y], core.at[dst_x, dst_y]))
            if round_ == 0:
                pairs.append((mats_rx.at[1, 1], mats_rx.at[place(direction)]))
        else:
            pairs.append((source.at[1 if dz > 0 else 0], edge.at[(*place(direction), 0 if dz > 0 else 1)]))
        return [
            pltpu.make_async_remote_copy(
                src_ref=src, dst_ref=dst, send_sem=halo_send.at[round_ + 2 * i, number],
                recv_sem=halo_recv.at[round_ + 2 * i, number],
                device_id=target(direction), device_id_type=pl.DeviceIdType.MESH,
            )
            for i, (src, dst) in enumerate(pairs)
        ]

    def halo_each(round_, act, incoming=False):
        for number, direction in enumerate(directions):
            @pl.when(exists(tuple(-step for step in direction) if incoming else direction))
            def _():
                for copy in halo_copies(round_, number):
                    act(copy)

    def halo_start(round_):
        halo_each(round_, lambda copy: copy.start())

    def halo_arrive(round_):
        halo_each(round_, lambda copy: copy.wait_recv(), True)

    def halo_left(round_):
        halo_each(round_, lambda copy: copy.wait_send())

    def each(count, body):
        if count <= 8:
            for k in range(1, count):
                body(k, 0)
        else:
            lax.fori_loop(1, count, body, 0)

    def group_of(axes):
        count, index = 1, 0
        for axis in axes:
            i = AXES.index(axis)
            count *= sizes[i]
            index = index * sizes[i] + me[i]
        return count, index

    def peer_id(axes, peer):
        coords = {axis: me[i] for i, axis in enumerate(AXES)}
        for axis in reversed(axes):
            size = sizes[AXES.index(axis)]
            coords[axis] = lax.rem(peer, size)
            peer = lax.div(peer, size)
        return coords

    offsets = []
    total_slots = 0
    for axes in phases:
        offsets.append(total_slots)
        total_slots += group_of(axes)[0]

    def fetch(x, y):
        return pltpu.make_async_copy(
            loads_ref.at[:, x, y, :], stack.at[x, y, pl.ds(0, cols), :], local_sems.at[0, x * ny + y]
        )

    def put(which, ref, x, y):
        return pltpu.make_async_copy(
            out_stage.at[which, x, y], ref.at[:, x, y, :], local_sems.at[1 + which, x * ny + y]
        )

    for x, y in own:
        fetch(x, y).start()

    for x in xs:
        for y in ys:
            if not (1 <= x <= nx and 1 <= y <= ny):
                padded[x, y] = jnp.zeros(padded.shape[2:], BF16)
                padded_im[x, y] = jnp.zeros(padded_im.shape[2:], BF16)
    for bx, by in itertools.product(range(3), repeat=2):
        mats_rx[bx, by] = jnp.zeros(mats_rx.shape[2:], F32)
        for side in range(2):
            ends_rx[bx, by, side] = jnp.zeros(ends_rx.shape[3:], BF16)
            ends_im_rx[bx, by, side] = jnp.zeros(ends_im_rx.shape[3:], BF16)

    barrier = pltpu.get_barrier_semaphore()
    expected = 0
    if len(phases) == 1:
        flat = sizes[0] * sizes[1]
        spot = me[0] * sizes[1] + me[1]
        for dz in (-1, 0, 1):
            good = True if dz == 0 else exists((0, 0, dz))

            def greet(k, carry, dz=dz):
                there = lax.rem(spot + k, flat)
                pl.semaphore_signal(
                    barrier, inc=1, device_id_type=pl.DeviceIdType.MESH,
                    device_id={"gx": lax.div(there, sizes[1]), "gy": lax.rem(there, sizes[1]), "gz": me[2] + dz},
                )
                return carry

            if dz == 0:
                each(flat, greet)
                expected = expected + flat - 1
            elif sizes[2] > 1:
                @pl.when(good)
                def _():
                    greet(0, 0)
                    each(flat, greet)
                expected = expected + jnp.where(good, flat, 0)
    else:
        for axes in phases:
            count, index = group_of(axes)

            def greet(k, carry, axes=axes, count=count, index=index):
                pl.semaphore_signal(barrier, inc=1, device_id=peer_id(axes, lax.rem(index + k, count)),
                                    device_id_type=pl.DeviceIdType.MESH)
                return carry

            each(count, greet)
            expected = expected + count - 1
        for direction in directions:
            good = exists(direction)

            @pl.when(good)
            def _():
                pl.semaphore_signal(barrier, inc=1, device_id=target(direction),
                                    device_id_type=pl.DeviceIdType.MESH)
            expected = expected + jnp.where(good, 1, 0)

    vouches = max(sizes[2] - 2, 0) if len(phases) == 1 else 0

    def vouch(round_):
        for dz in (-1, 1):
            @pl.when(exists((0, 0, dz)))
            def _():
                pl.semaphore_signal(vouch_sem.at[round_, 0 if dz > 0 else 1], inc=1, device_id=target((0, 0, dz)),
                                    device_id_type=pl.DeviceIdType.MESH)

    def vouched(round_):
        for dz in (-1, 1):
            @pl.when(exists((0, 0, dz)))
            def _():
                pl.semaphore_wait(vouch_sem.at[round_, 1 if dz > 0 else 0], 1)

    lane = lax.broadcasted_iota(jnp.int32, (1, LANES), 1)
    firsts = lasts = jnp.zeros((2 * cols, LANES), F32)
    for x in range(nx):
        mats_rx[1, 1, x * ny : (x + 1) * ny, :] = (mat_ref[x] + 1).astype(F32)
    for x, y in own:
        fetch(x, y).wait()
        values = stack[x, y, 0:cols, :]
        padded[x + 1, y + 1] = values.astype(BF16)
        row = x * ny + y
        ids = jnp.broadcast_to(mats_rx[1, 1, row : row + 1, :], (cols, nz))
        column = jnp.concatenate([values, ids], axis=0)
        firsts = jnp.where(lane == row, column[:, 0:1], firsts)
        lasts = jnp.where(lane == row, column[:, nz - 1 : nz], lasts)
    ends[0] = firsts.astype(BF16)
    ends[1] = lasts.astype(BF16)
    pl.semaphore_wait(barrier, expected)
    halo_start(0)
    if vouches:
        vouch(0)

    def block_of(x, y):
        bx, lx = (0, nx - 1) if x == 0 else (2, 0) if x == nx + 1 else (1, x - 1)
        by, ly = (0, ny - 1) if y == 0 else (2, 0) if y == ny + 1 else (1, y - 1)
        return bx, by, lx * ny + ly

    def merged(edge, x, y):
        bx, by, row = block_of(x, y)
        left, right = edge[bx, by, 0].astype(F32), edge[bx, by, 1].astype(F32)
        return jnp.where(lane == 0, right[:, row : row + 1],
                         jnp.where(lane == LANES - 1, left[:, row : row + 1], 0.0))

    def gram(left, right):
        total = None
        for x, y in own:
            part = dot(left(x, y), right(x, y), 1, 1)
            total = part if total is None else total + part
        return total

    def sum_copy(round_, number, k):
        axes = phases[number]
        count, index = group_of(axes)
        slot = offsets[number] + index
        return pltpu.make_async_remote_copy(
            src_ref=shares_of[round_].at[slot], dst_ref=shares_of[round_].at[slot],
            send_sem=sum_send.at[round_, offsets[number] + k], recv_sem=sum_recv.at[round_, offsets[number] + k],
            device_id=peer_id(axes, lax.rem(index + k, count)), device_id_type=pl.DeviceIdType.MESH,
        )

    def sum_arrival(round_, number, k):
        axes = phases[number]
        count, index = group_of(axes)
        source = lax.rem(index + count - k, count)
        slot = offsets[number] + source
        return pltpu.make_async_remote_copy(
            src_ref=shares_of[round_].at[slot], dst_ref=shares_of[round_].at[slot],
            send_sem=sum_send.at[round_, offsets[number] + k], recv_sem=sum_recv.at[round_, offsets[number] + k],
            device_id=peer_id(axes, lax.rem(index + k, count)), device_id_type=pl.DeviceIdType.MESH,
        )

    def sum_start(round_, number, tile):
        count, index = group_of(phases[number])
        shares_of[round_][offsets[number] + index] = tile

        def send(k, carry):
            sum_copy(round_, number, k).start()
            return carry

        each(count, send)

    def sum_finish(round_, number):
        count, _ = group_of(phases[number])

        def receive(k, carry):
            sum_arrival(round_, number, k).wait_recv()
            return carry

        each(count, receive)
        tile = shares_of[round_][offsets[number]]
        for peer in range(1, count):
            tile = tile + shares_of[round_][offsets[number] + peer]
        return tile

    def sum_turn(round_):
        for number in range(1, len(phases)):
            sum_start(round_, number, sum_finish(round_, number - 1))

    def sum_rest(round_):
        return unpack(sum_finish(round_, len(phases) - 1), cols)

    def sum_left(round_):
        for number, axes in enumerate(phases):
            def drain(k, carry, number=number):
                sum_copy(round_, number, k).wait_send()
                return carry

            each(group_of(axes)[0], drain)

    def loads_at(x, y):
        return stack[x, y, 0:cols, :]

    def image_at(x, y):
        return stack[x, y, cols:, :]

    def loads_at2(x, y):
        return stack2[x, y, 0:cols, :]

    def image_at2(x, y):
        return stack2[x, y, cols:, :]

    load_part = pack(gram(loads_at, loads_at))
    for round_ in range(1, vouches):
        vouched(round_ - 1)
        vouch(round_)
    halo_arrive(0)
    full = nz + LANES
    moduli = {}
    for x in xs:
        for y in ys:
            tail = merged(ends_rx, x, y)
            field[x, y] = jnp.concatenate([padded[x, y].astype(F32), tail[0:cols]], axis=1)
            bx, by, row = block_of(x, y)
            ids = jnp.concatenate([
                jnp.broadcast_to(mats_rx[bx, by, row : row + 1, :], (8, nz)), tail[cols : cols + 8]
            ], axis=1)
            modulus = jnp.zeros_like(ids)
            for number in range(mats):
                modulus = modulus + jnp.where(ids == float(number + 1), moduli_ref[number], 0.0)
            moduli[x, y] = modulus
    for x in range(nx + 1):
        for y in range(ny + 1):
            total = (moduli[x, y] + moduli[x, y + 1]) + (moduli[x + 1, y] + moduli[x + 1, y + 1])
            weight = 0.125 * (total + pltpu.roll(total, full - 1, 1))
            wt[x, y] = weight
            wtr[x, y] = pltpu.roll(weight, 1, 1)

    if vouches:
        vouched(vouches - 1)
    sum_start(0, 0, load_part)
    sum_turn(0)

    def double(tile):
        return jnp.concatenate([tile, tile], axis=0)

    def operate(direction_of, write):
        for x in range(nx):
            for y in range(ny):
                here = field[x + 1, y + 1]
                ahead = behind = flat = None
                w_ahead = w_behind = None
                for ex in (x, x + 1):
                    for ey in (y, y + 1):
                        corner_sum = (field[ex, ey] + field[ex, ey + 1]) + (field[ex + 1, ey] + field[ex + 1, ey + 1])
                        after, before = wt[ex, ey], wtr[ex, ey]
                        opposite = field[2 * ex - x, 2 * ey - y][:, 0:nz]
                        one = double(before) * corner_sum
                        two = double(after) * corner_sum
                        three = double((before + after)[:, 0:nz]) * opposite
                        ahead = one if ahead is None else ahead + one
                        behind = two if behind is None else behind + two
                        flat = three if flat is None else flat + three
                        w_ahead = before if w_ahead is None else w_ahead + before
                        w_behind = after if w_behind is None else w_behind + after
                ahead = ahead - double(w_ahead) * here
                behind = behind - double(w_behind) * here
                around = pltpu.roll(ahead, full - 1, 1)[:, 0:nz] + pltpu.roll(behind, 1, 1)[:, 0:nz] + flat
                centre = double((w_ahead + w_behind)[:, 0:nz]) * here[:, 0:nz]
                write(x, y, SIGMA * direction_of(x, y) + (k_far * around + k_self * centre))

    image_firsts = jnp.zeros((cols, LANES), F32)
    image_ends = [image_firsts, image_firsts]

    def write_first(x, y, image):
        stack[x, y, cols:, :] = image
        padded_im[x + 1, y + 1] = image.astype(BF16)
        row = x * ny + y
        image_ends[0] = jnp.where(lane == row, image[:, 0:1], image_ends[0])
        image_ends[1] = jnp.where(lane == row, image[:, nz - 1 : nz], image_ends[1])

    operate(loads_at, write_first)
    ends_im[0] = image_ends[0].astype(BF16)
    ends_im[1] = image_ends[1].astype(BF16)
    cross_part = gram(image_at, lambda x, y: stack[x, y])
    sum_start(1, 0, jnp.concatenate([pack(cross_part[:, 0:cols]), pack(cross_part[:, cols:])], axis=0))
    halo_start(1)
    square = sum_rest(0)
    sum_turn(1)
    row_id = lax.broadcasted_iota(jnp.int32, (cols, cols), 0)
    col_id = lax.broadcasted_iota(jnp.int32, (cols, cols), 1)
    eye = jnp.where(row_id == col_id, 1.0, 0.0)
    inverse = eliminate(square, eye)
    table = sum_rest(1)

    cross, quad = table[0:cols], table[cols:]
    alpha = eliminate(0.5 * (cross + cross.T), square)
    updated = square + dot(alpha, dot(quad, alpha, 1, 0) - cross, 0, 0) - dot(cross, alpha, 0, 0)
    beta = dot(inverse, updated, 1, 0)
    alpha_t = alpha.T
    mix = jnp.concatenate([(eye + beta).T, -alpha_t], axis=1)
    mix_hi = mix.astype(BF16)
    mix_lo = (mix - mix_hi.astype(F32)).astype(BF16)
    mix_both = jnp.concatenate([mix_hi, mix_lo], axis=0)

    halo_arrive(1)
    for x in xs:
        for y in ys:
            inner = 1 <= x <= nx and 1 <= y <= ny
            tail_l = merged(ends_rx, x, y)[0:cols].astype(BF16)
            tail_i = merged(ends_im_rx, x, y).astype(BF16)
            if inner:
                near = jnp.concatenate([tail_l, tail_i], axis=0)
            else:
                near = jnp.concatenate([
                    jnp.concatenate([padded[x, y], tail_l], axis=1),
                    jnp.concatenate([padded_im[x, y], tail_i], axis=1),
                ], axis=0)
            twice = dot(mix_both, near, 1, 0, None)
            mixed = twice[0:cols] + twice[cols:]
            if inner:
                direction = dot(mix, stack[x - 1, y - 1], 1, 0)
                stack2[x - 1, y - 1, 0:cols, :] = direction
                mixed = jnp.concatenate([direction, mixed], axis=1)
            field[x, y] = mixed.astype(BF16).astype(F32)

    def write_second(x, y, image):
        stack2[x, y, cols:, :] = image

    operate(loads_at2, write_second)
    sum_start(2, 0, pack(gram(image_at2, loads_at2)))
    for x, y in own:
        out_stage[0, x, y] = dot(alpha_t, stack[x, y, 0:cols, :], 1, 0)
        out_stage[1, x, y] = stack[x, y, 0:cols, :] - dot(alpha_t, stack[x, y, cols:, :], 1, 0)
    halo_left(0)
    halo_left(1)
    sum_left(0)
    sum_left(1)
    sum_turn(2)
    cross2 = sum_rest(2)
    alpha2_t = eliminate(0.5 * (cross2 + cross2.T), updated).T
    for x, y in own:
        out_stage[0, x, y] = out_stage[0, x, y] + dot(alpha2_t, stack2[x, y, 0:cols, :], 1, 0)
        put(0, sol_ref, x, y).start()
        out_stage[1, x, y] = out_stage[1, x, y] - dot(alpha2_t, stack2[x, y, cols:, :], 1, 0)
        put(1, res_ref, x, y).start()
    sum_left(2)
    for x, y in own:
        put(0, sol_ref, x, y).wait()
        put(1, res_ref, x, y).wait()


def on_device(sizes, loads, moduli, material):
    cols, nx, ny, nz = loads.shape
    count = int(np.prod(sizes))
    phases = (AXES,) if count <= DIRECT_LIMIT else (("gx", "gy"), ("gz",))
    slots = sum(int(np.prod([sizes[AXES.index(a)] for a in axes])) for axes in phases)
    body = functools.partial(kernel_body, sizes, phases, stiffness_values())
    out = pltpu.VMEM((cols, nx, ny, nz), F32)
    vmem = pl.BlockSpec(memory_space=pltpu.VMEM)
    anywhere = pl.BlockSpec(memory_space=pl.ANY)
    full = nz + LANES
    return pl.pallas_call(
        body,
        out_shape=(out, out),
        in_specs=[pl.BlockSpec(memory_space=pltpu.SMEM), anywhere, vmem],
        out_specs=(anywhere, anywhere),
        scratch_shapes=[
            pltpu.VMEM((nx, ny, 2 * cols, nz), F32),
            pltpu.VMEM((nx + 2, ny + 2, cols, nz), BF16),
            pltpu.VMEM((nx + 2, ny + 2, cols, nz), BF16),
            pltpu.VMEM((3, 3, nx * ny, nz), F32),
            pltpu.VMEM((2, 2 * cols, LANES), BF16),
            pltpu.VMEM((3, 3, 2, 2 * cols, LANES), BF16),
            pltpu.VMEM((2, cols, LANES), BF16),
            pltpu.VMEM((3, 3, 2, cols, LANES), BF16),
            pltpu.VMEM((nx + 2, ny + 2, cols, full), F32),
            pltpu.VMEM((nx + 1, ny + 1, 8, full), F32),
            pltpu.VMEM((nx + 1, ny + 1, 8, full), F32),
            pltpu.VMEM((nx, ny, 2 * cols, nz), F32),
            pltpu.VMEM((slots, cols * cols // LANES, LANES), F32),
            pltpu.VMEM((slots, 2 * cols * cols // LANES, LANES), F32),
            pltpu.VMEM((slots, cols * cols // LANES, LANES), F32),
            pltpu.SemaphoreType.DMA((3, 26)),
            pltpu.SemaphoreType.DMA((3, 26)),
            pltpu.SemaphoreType.DMA((3, slots)),
            pltpu.SemaphoreType.DMA((3, slots)),
            pltpu.VMEM((2, nx, ny, cols, nz), F32),
            pltpu.SemaphoreType.DMA((3, nx * ny)),
            pltpu.SemaphoreType.REGULAR((max(sizes[2], 2), 2)),
        ],
        compiler_params=pltpu.CompilerParams(collective_id=0, has_side_effects=True),
    )(moduli, loads, material)


def solution(mesh):
    sizes = tuple(mesh.shape[axis] for axis in AXES)
    in_specs = (P(None, "gx", "gy", "gz"), P(), P("gx", "gy", "gz"))
    out_specs = (P(None, "gx", "gy", "gz"), P(None, "gx", "gy", "gz"))
    return jax.shard_map(
        functools.partial(on_device, sizes), mesh=mesh, in_specs=in_specs, out_specs=out_specs, check_vma=False
    )
```
